256 devices in a mesh: section: 8 (over z), expert: 32 (over x, y, core).
Axes of the slice: x: 4, y: 4, z: 8, core: 2. Of those that a mesh axis runs over, the one named last changes fastest.
Arguments:
- tokens: bfloat16 [4, 4, 512, 1024], P(None, None, 'expert'), may hold values from -6 to 6
- expert_ids: int32 [8, 4, 4, 512, 2], P('section', None, None, 'expert'), may hold values from 0 to 7, as said below
- router_weight: float32 [8, 4, 1024, 8], P('section'), may hold values from -0.375 to 0.375
- w_gate: bfloat16 [8, 32, 1024, 1792], P('section', 'expert'), may hold values from -0.1875 to 0.1875
- w_up: bfloat16 [8, 32, 1024, 1792], P('section', 'expert'), may hold values from -0.1875 to 0.1875
- w_down: bfloat16 [8, 32, 1792, 1024], P('section', 'expert'), may hold values from -0.125 to 0.125
Outputs:
- layer_outputs: bfloat16 [8, 4, 4, 512, 1024], P('section', None, None, 'expert')
The draws below stay inside these ranges and needn't reach their ends.
Inputs may be any that keep to these rules, and one draw needn't show every extreme that they name: `expert_ids`: the two entries of a token are different experts. In each aligned block of 8 tokens (same layer, micro-batch and replica) no expert is named by more than 4 tokens, and some expert by exactly 4.
All inputs are finite; a program needn't handle non-finite values.
Results may differ from the reference program's by a relative error of at most 0.02.
Values may be sent and summed in bfloat16 or wider, within the bound.
A program may use at most 64 MiB of HBM per device.

```python
import jax
import jax.numpy as jnp
from jax import lax

D = 1024
FF = 1792
EXPERTS = 8
TOP = 2
TOK_DEV = 16
MICRO = 4
CAP = 4
REPS = 4
TOKENS = 512
LAYERS = 8
N_EXPERT = 32


def route_block(block_key, hot_expert, aligned):
    keys = jax.random.split(block_key, 5)
    block_rows = TOK_DEV // 2
    positions = jnp.arange(EXPERTS, dtype=jnp.int32)
    ordering = jax.random.permutation(keys[0], EXPERTS).astype(jnp.int32)
    moved = jnp.where(ordering == hot_expert, ordering[0], jnp.where(positions == 0, hot_expert, ordering))
    ordering = jnp.where(aligned, moved, ordering).astype(jnp.int32)
    double_full = jax.random.randint(keys[1], (), 0, 2, dtype=jnp.int32)
    ticket_count = EXPERTS * CAP
    labels = (jnp.arange(ticket_count, dtype=jnp.int32) // CAP).astype(jnp.int32)
    shuffled = jax.random.permutation(keys[2], ticket_count).astype(jnp.int32)
    ranking = jnp.argsort(shuffled, stable=True).astype(jnp.int32)
    forced = jnp.logical_or(labels == 0, jnp.logical_and(labels == 1, double_full == 1)).astype(jnp.int32)
    priority = (ranking + forced * ticket_count).astype(jnp.int32)
    selected = jnp.argsort(-priority, stable=True)[:2 * block_rows].astype(jnp.int32)
    picked = jnp.sort(labels[selected])
    named = ordering[picked]
    pairs = jnp.stack([named[:block_rows], named[block_rows:]], axis=-1)
    flips = jax.random.randint(keys[3], (block_rows, 1), 0, 2, dtype=jnp.int32)
    pairs = jnp.where(flips == 1, pairs[:, ::-1], pairs)
    rows_order = jax.random.permutation(keys[4], block_rows).astype(jnp.int32)
    return pairs[rows_order].astype(jnp.int32)


def draw_expert_ids(key, part):
    groups = LAYERS * MICRO * REPS
    block_rows = TOK_DEV // 2
    blocks = TOKENS // block_rows
    group_key = jax.random.fold_in(key, 7101)
    hot_all = jax.random.randint(jax.random.fold_in(group_key, 1), (groups,), 0, EXPERTS, dtype=jnp.int32)
    coin = jax.random.randint(jax.random.fold_in(group_key, 2), (LAYERS, MICRO, REPS), 0, 2, dtype=jnp.int32)
    micro_index = jnp.arange(MICRO, dtype=jnp.int32)[None, :, None]
    aligned_all = jnp.logical_or(coin == 1, micro_index == 0).reshape(groups)
    block_keys = jax.random.split(jax.random.fold_in(key, 7102), groups * blocks)
    hot_blocks = jnp.repeat(hot_all, blocks)
    aligned_blocks = jnp.repeat(aligned_all, blocks)
    result = jax.vmap(route_block)(block_keys, hot_blocks, aligned_blocks)
    return result.reshape(LAYERS, MICRO, REPS, TOKENS, TOP).astype(jnp.int32)


def level_of(rng, shape, cuts, low, largest):
    loudness = 1.0
    for axis_at, blocks in cuts:
        draws = jax.random.uniform(jax.random.fold_in(jax.random.fold_in(rng, 6), axis_at), (blocks,), jnp.float32, low / len(cuts), largest / len(cuts))
        loudness = loudness * jnp.repeat(jnp.exp(draws), shape[axis_at] // blocks).reshape((-1,) + (1,) * (len(shape) - 1 - axis_at))
    return loudness


def normal_values(stream_key, extent, width, most, pieces=(), held_as=jnp.bfloat16):
    entries = jax.random.normal(stream_key, extent, jnp.float32) * width
    if len(pieces) > 0:
        entries = level_of(stream_key, extent, pieces, -0.22, 0.18) * entries
    return jnp.clip(entries, min=-most, max=most).astype(held_as)


def setup_inputs(seed: int = 0) -> dict:
    splits = jax.random.split(jax.random.key(seed), 7)
    return {
        "tokens": normal_values(splits[0], (MICRO, REPS, TOKENS, D), 1.0, 6.0, ((2, 32),)),
        "expert_ids": draw_expert_ids(jax.random.fold_in(splits[6], 71), 0),
        "router_weight": normal_values(splits[2], (LAYERS, REPS, D, EXPERTS), (D // 4) ** -0.5, 0.375, ((0, 8),), jnp.float32),
        "w_gate": normal_values(splits[3], (LAYERS, N_EXPERT, D, FF), D ** -0.5, 0.1875, ((0, 8), (1, 32))),
        "w_up": normal_values(splits[4], (LAYERS, N_EXPERT, D, FF), D ** -0.5, 0.1875, ((0, 8), (1, 32))),
        "w_down": normal_values(splits[5], (LAYERS, N_EXPERT, FF, D), FF ** -0.5, 0.125, ((0, 8), (1, 32))),
    }


def normalize(hidden):
    values = hidden.astype(jnp.float32)
    return (values * lax.rsqrt(lax.optimization_barrier(jnp.mean(values * values, axis=-1, keepdims=True)) + 1e-06)).astype(jnp.bfloat16)

def expert_rows(inputs, gate_mat, up_mat, down_mat):
    gate_val = jnp.dot(inputs, gate_mat, preferred_element_type=jnp.float32)
    up_val = jnp.dot(inputs, up_mat, preferred_element_type=jnp.float32)
    inner = (jax.nn.silu(gate_val) * up_val).astype(jnp.bfloat16)
    return jnp.dot(inner, down_mat, preferred_element_type=jnp.float32).astype(jnp.bfloat16)

def reference(tokens, expert_ids, router_weight, w_gate, w_up, w_down):
    limit = MICRO * N_EXPERT * 2 * CAP
    hidden = tokens
    layer_list = []
    for layer in range(LAYERS):
        normed = normalize(hidden)
        logits = jnp.einsum('mrtd,rde->mrte', normed.astype(jnp.float32), router_weight[layer], precision=lax.Precision.HIGHEST)
        scores = jax.nn.sigmoid(logits)
        chosen = expert_ids[layer]
        picked = jnp.take_along_axis(scores, chosen, axis=-1)
        gates = picked / lax.optimization_barrier(jnp.sum(picked, axis=-1, keepdims=True))
        gate_layer = w_gate[layer]
        up_layer = w_up[layer]
        down_layer = w_down[layer]

        def one_replica(replica):
            rows_rep = lax.dynamic_index_in_dim(normed, replica, 1, keepdims=False).reshape(MICRO * TOKENS, D)
            ids_rep = lax.dynamic_index_in_dim(chosen, replica, 1, keepdims=False).reshape(-1)
            gates_rep = lax.dynamic_index_in_dim(gates, replica, 1, keepdims=False).reshape(-1)

            def one_expert(expert):
                member = ids_rep == expert
                order = jnp.argsort(jnp.where(member, 0, 1).astype(jnp.int32), stable=True)[:limit].astype(jnp.int32)
                source = (order // 2).astype(jnp.int32)
                instance = (replica * EXPERTS + expert).astype(jnp.int32)
                output = expert_rows(rows_rep[source], gate_layer[instance], up_layer[instance], down_layer[instance])
                weight = jnp.where(member[order], gates_rep[order], jnp.zeros_like(gates_rep[order]))
                return (source, weight[:, None] * output.astype(jnp.float32))
            sources, terms = lax.map(one_expert, jnp.arange(EXPERTS, dtype=jnp.int32))
            combined = jnp.zeros((MICRO * TOKENS, D), jnp.float32).at[sources.reshape(-1)].add(terms.reshape(-1, D))
            return combined.reshape(MICRO, TOKENS, D)
        combined = lax.map(one_replica, jnp.arange(REPS, dtype=jnp.int32))
        hidden = (hidden.astype(jnp.float32) + jnp.transpose(combined, (1, 0, 2, 3))).astype(jnp.bfloat16)
        layer_list.append(hidden)
    return jnp.stack(layer_list)
```

```python
import functools

import jax
import jax.numpy as jnp
from jax import lax
from jax.experimental import pallas as pl
from jax.experimental.pallas import tpu as pltpu
from jax.sharding import PartitionSpec as P

CAP = 4
BLOCK = 8
GROUPS = 2
TILE = 256
MESH = pl.DeviceIdType.MESH
F32 = jnp.float32
BF16 = jnp.bfloat16


def slot_columns(routes, place, slots):
    micro, reps, tok, top = routes.shape
    blocks = tok // BLOCK
    flat = routes.reshape(micro, reps, blocks, BLOCK * top)
    order = jnp.arange(BLOCK * top, dtype=jnp.int32)
    same = (flat[..., :, None] == flat[..., None, :]) & (order[None, :] < order[:, None])
    position = jnp.sum(same.astype(jnp.int32), axis=-1)
    block = place * blocks + jnp.arange(blocks, dtype=jnp.int32)
    columns = flat * slots + block[None, None, :, None] * CAP + position
    columns = columns.reshape(micro, reps, tok, top)
    return jnp.pad(jnp.swapaxes(columns, 0, 1), ((0, 0), (0, 0), (0, 0), (0, 128 - top)))


def router_parts(router, slots):
    parts, rest = [], router
    for _ in range(3):
        part = lax.reduce_precision(rest, 8, 7)
        rest = rest - part
        parts.append(jnp.repeat(part.astype(BF16), slots, axis=1))
    return jnp.concatenate(parts, axis=1)


def pipeline(
    sizes,
    tokens_ref,
    codes_ref,
    router_ref,
    gate_hbm,
    up_hbm,
    down_hbm,
    out_ref,
    w_gate,
    w_up,
    w_down,
    held,
    codes,
    gates,
    slot_send,
    slot_recv,
    inner,
    back_send,
    back_recv,
    result,
    weight_sem,
    code_sem,
    code_send_sem,
    token_send_sem,
    held_sem,
    slot_sem,
    slot_send_sem,
    back_sem,
    back_send_sem,
    next_send_sem,
    out_sem,
    out_send_sem,
):
    sections, experts, reps, micro, tok, width, hidden = sizes
    pieces = reps // GROUPS
    units = micro * pieces
    slots = GROUPS * tok // 2
    rows = experts * slots
    section = lax.axis_index("section")
    index = lax.axis_index("expert")
    column = index // experts
    mine = index % experts

    weights = [
        pltpu.make_async_copy(gate_hbm, w_gate, weight_sem.at[0]),
        pltpu.make_async_copy(up_hbm, w_up, weight_sem.at[1]),
        pltpu.make_async_copy(down_hbm, w_down, weight_sem.at[2]),
    ]
    for copy in weights:
        copy.start()

    barrier = pltpu.get_barrier_semaphore()

    def greet(at_section, at_index):
        pl.semaphore_signal(
            barrier, inc=1, device_id=(at_section, at_index), device_id_type=MESH
        )

    for step in range(1, experts):
        greet(section, column * experts + (mine + step) % experts)
    for step in range(1, reps):
        greet(section, (column + step) % reps * experts + mine)

    @pl.when(section > 0)
    def _():
        greet(section - 1, index)

    @pl.when(section < sections - 1)
    def _():
        greet(section + 1, index)

    below = jnp.where(section > 0, 1, 0)
    above = jnp.where(section < sections - 1, 1, 0)
    pl.semaphore_wait(barrier, experts - 1 + reps - 1 + below + above)

    @pl.when(section == 0)
    def _():
        for batch in range(micro):
            unit = batch * pieces + column // GROUPS
            place = pl.ds(column % GROUPS * tok, tok)
            for step in range(1, reps):
                rep = (column + step) % reps
                pltpu.make_async_remote_copy(
                    src_ref=tokens_ref.at[batch, rep],
                    dst_ref=held.at[unit, place],
                    send_sem=token_send_sem,
                    recv_sem=held_sem.at[unit],
                    device_id=(section, rep * experts + mine),
                    device_id_type=MESH,
                ).start()
            pltpu.make_async_copy(
                tokens_ref.at[batch, column], held.at[unit, place], held_sem.at[unit]
            ).start()

    for step in range(1, reps):
        rep = (column + step) % reps
        pltpu.make_async_remote_copy(
            src_ref=codes_ref.at[rep],
            dst_ref=codes.at[column],
            send_sem=code_send_sem,
            recv_sem=code_sem,
            device_id=(section, rep * experts + mine),
            device_id_type=MESH,
        ).start()
    pltpu.make_async_copy(codes_ref.at[column], codes.at[column], code_sem).start()
    pltpu.make_async_copy(codes_ref, codes, code_sem).wait()

    lanes = lax.broadcasted_iota(jnp.int32, (GROUPS * tok, rows), 1)

    def prepare(unit):
        pltpu.make_async_copy(held.at[unit], held.at[unit], held_sem.at[unit]).wait()
        values = held[unit].astype(F32)
        scale = lax.rsqrt(jnp.mean(values * values, axis=-1, keepdims=True) + 1e-06)
        normed = (values * scale).astype(BF16)
        logits = jnp.dot(normed, router_ref[...], preferred_element_type=F32)
        logits = (logits[:, :rows] + logits[:, rows : 2 * rows]) + logits[:, 2 * rows :]
        batch, piece = unit // pieces, unit % pieces
        code = jnp.concatenate(
            [codes[piece * GROUPS + group, batch] for group in range(GROUPS)], axis=0
        )
        chosen = (code[:, 0:1] == lanes) | (code[:, 1:2] == lanes)
        picked = jnp.where(chosen, jax.nn.sigmoid(logits), 0.0)
        gates[unit] = picked / jnp.sum(picked, axis=-1, keepdims=True)
        placing = jnp.where(chosen, 1.0, 0.0).astype(BF16)
        filled = lax.dot_general(
            placing, normed, (((0,), (0,)), ((), ())), preferred_element_type=F32
        )
        slot_send[unit] = filled.astype(BF16).reshape(experts, slots, width)
        slot_recv[unit, mine] = slot_send[unit, mine]
        for step in range(1, experts):
            peer = (mine + step) % experts
            pltpu.make_async_remote_copy(
                src_ref=slot_send.at[unit, peer],
                dst_ref=slot_recv.at[unit, mine],
                send_sem=slot_send_sem,
                recv_sem=slot_sem.at[unit],
                device_id=(section, column * experts + peer),
                device_id_type=MESH,
            ).start()

    def serve(unit):
        @pl.when(unit == 0)
        def _():
            for copy in weights:
                copy.wait()

        others = slot_recv.at[unit, pl.ds(0, experts - 1)]
        pltpu.make_async_copy(others, others, slot_sem.at[unit]).wait()
        given = slot_recv[unit].reshape(rows, width)
        for tile in range(hidden // TILE):
            part = slice(tile * TILE, (tile + 1) * TILE)
            gate_val = jnp.dot(given, w_gate[:, part], preferred_element_type=F32)
            up_val = jnp.dot(given, w_up[:, part], preferred_element_type=F32)
            inner[:, part] = (jax.nn.silu(gate_val) * up_val).astype(BF16)
        for tile in range(width // TILE):
            part = slice(tile * TILE, (tile + 1) * TILE)
            answer = jnp.dot(inner[...], w_down[:, part], preferred_element_type=F32)
            back_send[unit, :, :, part] = answer.astype(BF16).reshape(experts, slots, TILE)
        back_recv[unit, mine] = back_send[unit, mine]
        for step in range(1, experts):
            peer = (mine + step) % experts
            pltpu.make_async_remote_copy(
                src_ref=back_send.at[unit, peer],
                dst_ref=back_recv.at[unit, mine],
                send_sem=back_send_sem,
                recv_sem=back_sem.at[unit],
                device_id=(section, column * experts + peer),
                device_id_type=MESH,
            ).start()

    def combine(unit):
        others = back_recv.at[unit, pl.ds(0, experts - 1)]
        pltpu.make_async_copy(others, others, back_sem.at[unit]).wait()
        answers = back_recv[unit].reshape(rows, width)
        weight = gates[unit]
        high = weight.astype(BF16)
        low = (weight - high.astype(F32)).astype(BF16)
        total = jnp.dot(high, answers, preferred_element_type=F32)
        total = total + jnp.dot(low, answers, preferred_element_type=F32)
        result[unit] = (held[unit].astype(F32) + total).astype(BF16)

        @pl.when(section < sections - 1)
        def _():
            pltpu.make_async_remote_copy(
                src_ref=result.at[unit],
                dst_ref=held.at[unit],
                send_sem=next_send_sem,
                recv_sem=held_sem.at[unit],
                device_id=(section + 1, index),
                device_id_type=MESH,
            ).start()

        batch, piece = unit // pieces, unit % pieces
        for group in range(GROUPS):
            owner = piece * GROUPS + group
            source = result.at[unit, pl.ds(group * tok, tok)]
            target = out_ref.at[0, batch, column]

            @pl.when(owner == column)
            def _():
                pltpu.make_async_copy(source, target, out_sem).start()

            @pl.when(owner != column)
            def _():
                pltpu.make_async_remote_copy(
                    src_ref=source,
                    dst_ref=target,
                    send_sem=out_send_sem,
                    recv_sem=out_sem,
                    device_id=(section, owner * experts + mine),
                    device_id_type=MESH,
                ).start()

    def tick(now, carry):
        @pl.when(now < units)
        def _():
            prepare(now)

        @pl.when(jnp.logical_and(now >= 1, now < units + 1))
        def _():
            serve(now - 1)

        @pl.when(now >= 2)
        def _():
            combine(now - 2)

        return carry

    lax.fori_loop(0, units + 2, tick, 0)

    def drain(ref, sem):
        pltpu.make_async_copy(ref, ref, sem).wait()

    drain(codes.at[pl.ds(0, reps - 1)], code_send_sem)
    drain(slot_send.at[:, pl.ds(0, experts - 1)], slot_send_sem)
    drain(back_send.at[:, pl.ds(0, experts - 1)], back_send_sem)

    @pl.when(section == 0)
    def _():
        drain(out_ref.at[0, :, pl.ds(0, reps - 1)], token_send_sem)

    @pl.when(section < sections - 1)
    def _():
        drain(result, next_send_sem)

    drain(out_ref.at[0, :, pl.ds(0, reps - 1)], out_send_sem)
    drain(out_ref, out_sem)


def per_device(tokens, expert_ids, router_weight, w_gate, w_up, w_down):
    micro, reps, tok, width = tokens.shape
    hidden = w_gate.shape[3]
    sections = lax.axis_size("section")
    experts = lax.axis_size("expert") // reps
    units = micro * reps // GROUPS
    unit_rows = GROUPS * tok
    slots = unit_rows // 2
    rows = experts * slots
    column = lax.axis_index("expert") // experts
    codes = slot_columns(expert_ids[0], column % GROUPS, slots)
    router = router_parts(
        lax.dynamic_index_in_dim(router_weight[0], column, 0, keepdims=False), slots
    )
    sizes = (sections, experts, reps, micro, tok, width, hidden)
    anywhere = pl.BlockSpec(memory_space=pl.ANY)
    local = pl.BlockSpec(memory_space=pltpu.VMEM)
    dma = pltpu.SemaphoreType.DMA
    exchange = pltpu.VMEM((units, experts, slots, width), BF16)
    return pl.pallas_call(
        functools.partial(pipeline, sizes),
        out_shape=jax.ShapeDtypeStruct((1, micro, reps, tok, width), BF16),
        in_specs=[anywhere, anywhere, local, anywhere, anywhere, anywhere],
        out_specs=anywhere,
        scratch_shapes=[
            pltpu.VMEM((width, hidden), BF16),
            pltpu.VMEM((width, hidden), BF16),
            pltpu.VMEM((hidden, width), BF16),
            pltpu.VMEM((units, unit_rows, width), BF16),
            pltpu.VMEM((reps, micro, tok, 128), jnp.int32),
            pltpu.VMEM((units, unit_rows, rows), F32),
            exchange,
            exchange,
            pltpu.VMEM((rows, hidden), BF16),
            exchange,
            exchange,
            pltpu.VMEM((units, unit_rows, width), BF16),
            dma((3,)),
            dma,
            dma,
            dma,
            dma((units,)),
            dma((units,)),
            dma,
            dma((units,)),
            dma,
            dma,
            dma,
            dma,
        ],
        compiler_params=pltpu.CompilerParams(
            collective_id=0, has_side_effects=True, vmem_limit_bytes=52 * 1024 * 1024
        ),
    )(tokens, codes, router, w_gate[0, 0], w_up[0, 0], w_down[0, 0])


def solution(mesh):
    in_specs = (
        P(None, None, "expert", None),
        P("section", None, None, "expert", None),
        P("section", None, None, None),
        P("section", "expert", None, None),
        P("section", "expert", None, None),
        P("section", "expert", None, None),
    )
    out_specs = P("section", None, None, "expert", None)
    return jax.shard_map(
        per_device, mesh=mesh, in_specs=in_specs, out_specs=out_specs, check_vma=False
    )
```

```python
import functools

import jax
import jax.numpy as jnp
from jax import lax
from jax.experimental import pallas as pl
from jax.experimental.pallas import tpu as pltpu
from jax.sharding import PartitionSpec as P

CAP = 4
BLOCK = 8
SERVE = 1
COMBINE = 2
TILE = 256
PARTS = 2
MESH = pl.DeviceIdType.MESH
F32 = jnp.float32
BF16 = jnp.bfloat16


def chosen_lanes(routes):
    micro, reps, tok, top = routes.shape
    named = jnp.transpose(routes, (1, 2, 0, 3)).reshape(reps, tok, micro * top)
    return jnp.pad(named.astype(F32), ((0, 0), (0, 0), (0, 128 - micro * top)))


def pipeline(
    sizes,
    tokens_ref,
    routes_ref,
    router_ref,
    gate_hbm,
    up_hbm,
    down_hbm,
    out_ref,
    w_gate,
    w_up,
    w_down,
    held,
    routes,
    router_raw,
    router,
    gates,
    slot_send,
    slot_recv,
    inner,
    back_send,
    back_recv,
    result,
    weight_sem,
    router_sem,
    route_sem,
    route_send_sem,
    token_send_sem,
    held_sem,
    slot_sem,
    slot_send_sem,
    back_sem,
    back_send_sem,
    next_send_sem,
    out_sem,
    out_send_sem,
):
    sections, experts, reps, micro, tok, width, hidden = sizes
    units = micro * reps
    slots = tok // 2
    rows = experts * slots
    section = lax.axis_index("section")
    index = lax.axis_index("expert")
    column = index // experts
    mine = index % experts
    far_first = sorted(range(1, experts), key=lambda step: -min(step, experts - step))

    router_copy = pltpu.make_async_copy(router_ref.at[column], router_raw, router_sem)
    router_copy.start()
    weights = [
        pltpu.make_async_copy(gate_hbm, w_gate, weight_sem.at[0]),
        pltpu.make_async_copy(up_hbm, w_up, weight_sem.at[1]),
        pltpu.make_async_copy(down_hbm, w_down, weight_sem.at[2]),
    ]
    barrier = pltpu.get_barrier_semaphore()

    def greet(at_section, at_index):
        pl.semaphore_signal(
            barrier, inc=1, device_id=(at_section, at_index), device_id_type=MESH
        )

    for step in range(1, experts):
        greet(section, column * experts + (mine + step) % experts)
    for step in range(1, reps):
        greet(section, (column + step) % reps * experts + mine)

    @pl.when(section > 0)
    def _():
        greet(section - 1, index)

    @pl.when(section < sections - 1)
    def _():
        greet(section + 1, index)

    below = jnp.where(section > 0, 1, 0)
    above = jnp.where(section < sections - 1, 1, 0)
    pl.semaphore_wait(barrier, experts - 1 + reps - 1 + below + above)

    def spread_tokens(batch):
        unit = batch * reps + column
        for step in range(1, reps):
            rep = (column + step) % reps
            pltpu.make_async_remote_copy(
                src_ref=tokens_ref.at[batch, rep],
                dst_ref=held.at[unit],
                send_sem=token_send_sem,
                recv_sem=held_sem.at[unit],
                device_id=(section, rep * experts + mine),
                device_id_type=MESH,
            ).start()
        pltpu.make_async_copy(
            tokens_ref.at[batch, column], held.at[unit], held_sem.at[unit]
        ).start()

    @pl.when(section == 0)
    def _():
        spread_tokens(0)

    for step in range(1, reps):
        rep = (column + step) % reps
        pltpu.make_async_remote_copy(
            src_ref=routes_ref.at[rep],
            dst_ref=routes.at[column],
            send_sem=route_send_sem,
            recv_sem=route_sem,
            device_id=(section, rep * experts + mine),
            device_id_type=MESH,
        ).start()

    @pl.when(section == 0)
    def _():
        for batch in range(1, micro):
            spread_tokens(batch)

    for copy in weights:
        copy.start()

    routes[column] = routes_ref[column]
    router_copy.wait()
    shift = slots.bit_length() - 1
    spread = lax.broadcasted_iota(jnp.int32, (rows, experts), 1) == jnp.right_shift(
        lax.broadcasted_iota(jnp.int32, (rows, experts), 0), shift
    )
    spread = jnp.where(spread, 1.0, 0.0).astype(BF16)
    rest = router_raw[...]
    for part in range(3):
        piece = rest.astype(BF16)
        rest = rest - piece.astype(F32)
        router[part * rows : (part + 1) * rows, :] = jnp.dot(
            spread, piece, preferred_element_type=F32
        ).astype(BF16)

    lanes = lax.broadcasted_iota(jnp.int32, (tok, 128), 1)
    columns = lax.broadcasted_iota(jnp.int32, (tok, rows), 1)
    expert_lane = jnp.right_shift(columns, shift).astype(F32)
    block_row = jnp.right_shift(lax.broadcasted_iota(jnp.int32, (tok, rows), 0), 3)
    rank_lane = (jnp.bitwise_and(columns, slots - 1) - block_row * CAP).astype(F32)
    row = lax.broadcasted_iota(jnp.int32, (tok, tok), 0)
    earlier = lax.broadcasted_iota(jnp.int32, (tok, tok), 1)
    earlier = (earlier < row) & (jnp.right_shift(earlier, 3) == jnp.right_shift(row, 3))
    earlier = jnp.where(earlier, 1.0, 0.0).astype(BF16)

    others = routes.at[pl.ds(0, reps - 1)]
    pltpu.make_async_copy(others, others, route_sem).wait()

    def prepare(unit):
        batch, origin = unit // reps, unit % reps
        route = routes[origin]
        first = jnp.sum(jnp.where(lanes == 2 * batch, route, 0.0), axis=-1, keepdims=True)
        second = jnp.sum(jnp.where(lanes == 2 * batch + 1, route, 0.0), axis=-1, keepdims=True)
        named = (first == expert_lane) | (second == expert_lane)
        rank = jnp.dot(
            earlier, jnp.where(named, 1.0, 0.0).astype(BF16), preferred_element_type=F32
        )
        chosen = jnp.where(named & (rank == rank_lane), 1.0, 0.0)
        placing = chosen.astype(BF16)

        pltpu.make_async_copy(held.at[unit], held.at[unit], held_sem.at[unit]).wait()
        values = held[unit].astype(F32)
        scale = lax.rsqrt(jnp.mean(values * values, axis=-1, keepdims=True) + 1e-06)
        normed = (values * scale).astype(BF16)
        filled = lax.dot_general(
            placing, normed, (((0,), (0,)), ((), ())), preferred_element_type=F32
        )
        slot_send[unit] = filled.astype(BF16).reshape(experts, slots, width)
        for step in far_first:
            peer = (mine + step) % experts
            pltpu.make_async_remote_copy(
                src_ref=slot_send.at[unit, peer],
                dst_ref=slot_recv.at[unit, mine],
                send_sem=slot_send_sem,
                recv_sem=slot_sem.at[unit],
                device_id=(section, column * experts + peer),
                device_id_type=MESH,
            ).start()
        slot_recv[unit, mine] = slot_send[unit, mine]
        logits = lax.dot_general(
            normed, router[...], (((1,), (1,)), ((), ())), preferred_element_type=F32
        )
        logits = (logits[:, :rows] + logits[:, rows : 2 * rows]) + logits[:, 2 * rows :]
        picked = jnp.where(chosen > 0.0, jax.nn.sigmoid(logits), 0.0)
        gates[unit] = picked / jnp.sum(picked, axis=-1, keepdims=True)

    def serve(unit):
        @pl.when(unit == 0)
        def _():
            for copy in weights:
                copy.wait()

        sent = slot_recv.at[unit, pl.ds(0, experts - 1)]
        pltpu.make_async_copy(sent, sent, slot_sem.at[unit]).wait()
        given = slot_recv[unit].reshape(rows, width)
        for tile in range(hidden // TILE):
            part = slice(tile * TILE, (tile + 1) * TILE)
            gate_val = jnp.dot(given, w_gate[:, part], preferred_element_type=F32)
            up_val = jnp.dot(given, w_up[:, part], preferred_element_type=F32)
            inner[:, part] = (jax.nn.silu(gate_val) * up_val).astype(BF16)
        half = width // PARTS
        for start in range(0, width, half):
            for tile in range(start, start + half, TILE):
                part = slice(tile, tile + TILE)
                answer = jnp.dot(inner[...], w_down[:, part], preferred_element_type=F32)
                back_send[unit, :, :, part] = answer.astype(BF16).reshape(experts, slots, TILE)
            for step in far_first:
                peer = (mine + step) % experts
                pltpu.make_async_remote_copy(
                    src_ref=back_send.at[unit, peer, :, pl.ds(start, half)],
                    dst_ref=back_recv.at[unit, mine, :, pl.ds(start, half)],
                    send_sem=back_send_sem,
                    recv_sem=back_sem.at[unit],
                    device_id=(section, column * experts + peer),
                    device_id_type=MESH,
                ).start()
        back_recv[unit, mine] = back_send[unit, mine]

    def combine(unit):
        sent = back_recv.at[unit, pl.ds(0, experts - 1)]
        pltpu.make_async_copy(sent, sent, back_sem.at[unit]).wait()
        answers = back_recv[unit].reshape(rows, width)
        weight = gates[unit]
        high = weight.astype(BF16)
        low = (weight - high.astype(F32)).astype(BF16)
        total = jnp.dot(high, answers, preferred_element_type=F32)
        total = total + jnp.dot(low, answers, preferred_element_type=F32)
        result[unit] = (held[unit].astype(F32) + total).astype(BF16)

        @pl.when(section < sections - 1)
        def _():
            pltpu.make_async_remote_copy(
                src_ref=result.at[unit],
                dst_ref=held.at[unit],
                send_sem=next_send_sem,
                recv_sem=held_sem.at[unit],
                device_id=(section + 1, index),
                device_id_type=MESH,
            ).start()

        batch, owner = unit // reps, unit % reps
        target = out_ref.at[0, batch, column]

        @pl.when(owner == column)
        def _():
            pltpu.make_async_copy(result.at[unit], target, out_sem).start()

        @pl.when(owner != column)
        def _():
            pltpu.make_async_remote_copy(
                src_ref=result.at[unit],
                dst_ref=target,
                send_sem=out_send_sem,
                recv_sem=out_sem,
                device_id=(section, owner * experts + mine),
                device_id_type=MESH,
            ).start()

    def at(unit, stage):
        @pl.when(jnp.logical_and(unit >= 0, unit < units))
        def _():
            stage(unit)

    def tick(now, carry):
        at(now, prepare)
        at(now - SERVE, serve)
        at(now - COMBINE, combine)
        return carry

    lax.fori_loop(0, units + COMBINE, tick, 0)

    def drain(ref, sem):
        pltpu.make_async_copy(ref, ref, sem).wait()

    drain(others, route_send_sem)
    drain(slot_send.at[:, pl.ds(0, experts - 1)], slot_send_sem)
    drain(back_send.at[:, pl.ds(0, experts - 1)], back_send_sem)

    @pl.when(section == 0)
    def _():
        drain(out_ref.at[0, :, pl.ds(0, reps - 1)], token_send_sem)

    @pl.when(section < sections - 1)
    def _():
        drain(result, next_send_sem)

    drain(out_ref.at[0, :, pl.ds(0, reps - 1)], out_send_sem)
    drain(out_ref, out_sem)


def per_device(tokens, expert_ids, router_weight, w_gate, w_up, w_down):
    micro, reps, tok, width = tokens.shape
    hidden = w_gate.shape[3]
    sections = lax.axis_size("section")
    experts = lax.axis_size("expert") // reps
    units = micro * reps
    slots = tok // 2
    rows = experts * slots
    routes = chosen_lanes(expert_ids[0])
    sizes = (sections, experts, reps, micro, tok, width, hidden)
    anywhere = pl.BlockSpec(memory_space=pl.ANY)
    local = pl.BlockSpec(memory_space=pltpu.VMEM)
    dma = pltpu.SemaphoreType.DMA
    exchange = pltpu.VMEM((units, experts, slots, width), BF16)
    return pl.pallas_call(
        functools.partial(pipeline, sizes),
        out_shape=jax.ShapeDtypeStruct((1, micro, reps, tok, width), BF16),
        in_specs=[anywhere, local, anywhere, anywhere, anywhere, anywhere],
        out_specs=anywhere,
        scratch_shapes=[
            pltpu.VMEM((width, hidden), BF16),
            pltpu.VMEM((width, hidden), BF16),
            pltpu.VMEM((hidden, width), BF16),
            pltpu.VMEM((units, tok, width), BF16),
            pltpu.VMEM((reps, tok, 128), F32),
            pltpu.VMEM((experts, width), F32),
            pltpu.VMEM((3 * rows, width), BF16),
            pltpu.VMEM((units, tok, rows), F32),
            exchange,
            exchange,
            pltpu.VMEM((rows, hidden), BF16),
            exchange,
            exchange,
            pltpu.VMEM((units, tok, width), BF16),
            dma((3,)),
            dma,
            dma,
            dma,
            dma,
            dma((units,)),
            dma((units,)),
            dma,
            dma((units,)),
            dma,
            dma,
            dma,
            dma,
        ],
        compiler_params=pltpu.CompilerParams(
            collective_id=0, has_side_effects=True, vmem_limit_bytes=52 * 1024 * 1024
        ),
    )(tokens, routes, jnp.swapaxes(router_weight[0], 1, 2), w_gate[0, 0], w_up[0, 0], w_down[0, 0])


def solution(mesh):
    in_specs = (
        P(None, None, "expert", None),
        P("section", None, None, "expert", None),
        P("section", None, None, None),
        P("section", "expert", None, None),
        P("section", "expert", None, None),
        P("section", "expert", None, None),
    )
    out_specs = P("section", None, None, "expert", None)
    return jax.shard_map(
        per_device, mesh=mesh, in_specs=in_specs, out_specs=out_specs, check_vma=False
    )
```
